32 devices in a mesh: ep: 4 (over y, x), fsdp: 8 (over z, core).
Axes of the slice: x: 2, y: 2, z: 4, core: 2. Of those that a mesh axis runs over, the one named last changes fastest.
Arguments:
- w_gate: float32 [64, 2048, 1024], P('ep', 'fsdp'), may hold values from -0.1875 to 0.1875
- avg_gate: bfloat16 [64, 2048, 1024], P('ep', 'fsdp'), may hold values from -0.0625 to 0.0625
- w_up: float32 [64, 2048, 1024], P('ep', 'fsdp'), may hold values from -0.1875 to 0.1875
- avg_up: bfloat16 [64, 2048, 1024], P('ep', 'fsdp'), may hold values from -0.0625 to 0.0625
- w_down: float32 [64, 1024, 2048], P('ep', None, 'fsdp'), may hold values from -0.25 to 0.25
- avg_down: bfloat16 [64, 1024, 2048], P('ep', None, 'fsdp'), may hold values from -0.09375 to 0.09375
- router_weight: float32 [2048, 64], P('fsdp', 'ep'), may hold values from -0.125 to 0.125
- router_gain: float32 [2048], P('fsdp'), may hold values from 0.25 to 1.75
Outputs:
- serve_gate: bfloat16 [64, 2048, 1024], P('ep', None, 'fsdp')
- serve_up: bfloat16 [64, 2048, 1024], P('ep', None, 'fsdp')
- serve_down: bfloat16 [64, 1024, 2048], P('ep', 'fsdp')
- scale_gate: float32 [64, 1024], P('ep', 'fsdp')
- scale_up: float32 [64, 1024], P('ep', 'fsdp')
- scale_down: float32 [64, 1024], P('ep', 'fsdp')
- serve_router: bfloat16 [2048, 64], replicated
The draws below stay inside these ranges and needn't reach their ends.
All inputs are finite; a program needn't handle non-finite values.
Results may differ from the reference program's by a relative error of at most 0.001.
Values may be sent and summed in bfloat16 or wider, within the bound.
A program may use at most 192 MiB of HBM per device.

```python
import jax
import jax.numpy as jnp
from jax import lax

EXPERTS = 64
D_MODEL = 2048
D_EXPERT = 1024


def with_spikes(result, stream_key, source, target, blocks, factor):
    owner, partner = [(jnp.arange(result.shape[axis_at]) // (result.shape[axis_at] // blocks)).reshape([-1 if axis == axis_at else 1 for axis in range(result.ndim)]) for axis_at in (source, target)]
    chosen = jax.random.permutation(stream_key, blocks)[partner]
    strong = (owner == chosen) | (owner == (partner + blocks // 2) % blocks)
    return jnp.where(strong, factor * result, result)


def levels(rng, shape, split, least, top_value):
    gain, own = 1.0, jax.random.fold_in(rng, 6)
    for position, shards_of in split:
        steps = jnp.exp(jax.random.uniform(jax.random.fold_in(own, position), (shards_of,), jnp.float32, least / len(split), top_value / len(split)))
        gain = gain * jnp.repeat(steps, shape[position] // shards_of).reshape([-1 if axis == position else 1 for axis in range(len(shape))])
    return gain


def centred(rng, dims, width, bound, cuts=(), kind=jnp.bfloat16):
    drawn = jax.random.normal(rng, dims, jnp.float32) * width
    if len(cuts) > 0:
        drawn = levels(rng, dims, cuts, -0.22, 0.18) * drawn
    return jnp.clip(drawn, min=-bound, max=bound).astype(kind)


def gaussian_with(stream_key, shape, spread, reach, split, heavy, dtype=jnp.bfloat16):
    values = spread * jax.random.normal(stream_key, shape, jnp.float32)
    if split:
        values = values * levels(stream_key, shape, split, -0.22, 0.18)
    return jnp.clip(with_spikes(values, jax.random.fold_in(stream_key, 3), *heavy), -reach, reach).astype(dtype)


def setup_inputs(seed: int = 0) -> dict:
    splits = jax.random.split(jax.random.key(seed), 9)
    w_gate = gaussian_with(splits[0], (EXPERTS, D_MODEL, D_EXPERT), D_MODEL ** -0.5, 0.1875, ((0, 4), (1, 8)), (1, 2, 8, 2.0), jnp.float32)
    avg_gate = centred(splits[1], (EXPERTS, D_MODEL, D_EXPERT), (D_MODEL * 4) ** -0.5, 0.0625, ((0, 4), (1, 8)))
    w_up = gaussian_with(splits[2], (EXPERTS, D_MODEL, D_EXPERT), D_MODEL ** -0.5, 0.1875, ((0, 4), (1, 8)), (1, 2, 8, 2.0), jnp.float32)
    avg_up = centred(splits[3], (EXPERTS, D_MODEL, D_EXPERT), (D_MODEL * 4) ** -0.5, 0.0625, ((0, 4), (1, 8)))
    w_down = gaussian_with(splits[4], (EXPERTS, D_EXPERT, D_MODEL), D_EXPERT ** -0.5, 0.25, ((0, 4), (2, 8)), (2, 1, 8, 2.0), jnp.float32)
    avg_down = centred(splits[5], (EXPERTS, D_EXPERT, D_MODEL), (D_EXPERT * 4) ** -0.5, 0.09375, ((0, 4), (2, 8)))
    router_weight = centred(splits[6], (D_MODEL, EXPERTS), D_MODEL ** -0.5, 0.125, ((0, 8), (1, 4)), jnp.float32)
    router_gain = jnp.clip(1.0 + 0.15 * jax.random.normal(splits[7], (D_MODEL,), jnp.float32), 0.25, 1.75)
    return {"w_gate": w_gate, "avg_gate": avg_gate, "w_up": w_up, "avg_up": avg_up, "w_down": w_down, "avg_down": avg_down, "router_weight": router_weight, "router_gain": router_gain}


def reference(w_gate, avg_gate, w_up, avg_up, w_down, avg_down, router_weight, router_gain):
    fresh_gate = w_gate + avg_gate.astype(jnp.float32)
    fresh_up = w_up + avg_up.astype(jnp.float32)
    fresh_down = w_down + avg_down.astype(jnp.float32)
    scale_gate = jnp.sqrt(lax.optimization_barrier(jnp.sum(fresh_gate * fresh_gate, axis=1)))
    serve_gate = (fresh_gate / jnp.expand_dims(scale_gate, 1)).astype(jnp.bfloat16)
    scale_up = jnp.sqrt(lax.optimization_barrier(jnp.sum(fresh_up * fresh_up, axis=1)))
    serve_up = (fresh_up / jnp.expand_dims(scale_up, 1)).astype(jnp.bfloat16)
    scale_down = jnp.sqrt(lax.optimization_barrier(jnp.sum(fresh_down * fresh_down, axis=2)))
    serve_down = (fresh_down / jnp.expand_dims(scale_down, 2)).astype(jnp.bfloat16)
    serve_router = (router_weight * router_gain[:, None]).astype(jnp.bfloat16)
    return (serve_gate, serve_up, serve_down, scale_gate, scale_up, scale_down, serve_router)
```

```python
import jax
import jax.numpy as jnp
from jax import lax
from jax.experimental import pallas as pl
from jax.sharding import PartitionSpec as P


def fresh_of(w, avg):
    return w + avg.astype(jnp.float32)


def narrow_of(w, avg, total, axis):
    return (fresh_of(w, avg) / jnp.expand_dims(jnp.sqrt(total), axis)).astype(jnp.bfloat16)


def squares(w, avg, axis):
    fresh = fresh_of(w, avg)
    return jnp.sum(fresh * fresh, axis=axis)


def exchange(x):
    return lax.all_to_all(x, "fsdp", split_axis=0, concat_axis=0, tiled=True)


def sum_kernel(w_ref, avg_ref, total_ref):
    fresh = w_ref[0] + avg_ref[0].astype(jnp.float32)
    total_ref[0] = jnp.sum(fresh * fresh, axis=0, keepdims=True)


def piece_kernel(n, w_ref, avg_ref, total_ref, out_ref):
    width = w_ref.shape[2] // n
    for k in range(n):
        at = slice(k * width, (k + 1) * width)
        fresh = w_ref[0, :, at] + avg_ref[0, :, at].astype(jnp.float32)
        out_ref[k, 0] = (fresh / jnp.sqrt(total_ref[0, :, at])).astype(jnp.bfloat16)


def column_squares(w, avg):
    experts, depth, width = w.shape
    block = pl.BlockSpec((1, depth, width), lambda e: (e, 0, 0))
    total = pl.pallas_call(
        sum_kernel,
        grid=(experts,),
        in_specs=[block, block],
        out_specs=pl.BlockSpec((1, 1, width), lambda e: (e, 0, 0)),
        out_shape=jax.ShapeDtypeStruct((experts, 1, width), jnp.float32),
        cost_estimate=pl.CostEstimate(flops=3 * w.size, bytes_accessed=6 * w.size, transcendentals=0),
    )(w, avg)
    return total.reshape(experts, width)


def column_pieces(w, avg, total):
    n = lax.axis_size("fsdp")
    experts, depth, width = w.shape
    block = pl.BlockSpec((1, depth, width), lambda e: (e, 0, 0))
    return pl.pallas_call(
        lambda *refs: piece_kernel(n, *refs),
        grid=(experts,),
        in_specs=[block, block, pl.BlockSpec((1, 1, width), lambda e: (e, 0, 0))],
        out_specs=pl.BlockSpec((n, 1, depth, width // n), lambda e: (0, e, 0, 0)),
        out_shape=jax.ShapeDtypeStruct((n, experts, depth, width // n), jnp.bfloat16),
        cost_estimate=pl.CostEstimate(flops=3 * w.size, bytes_accessed=8 * w.size, transcendentals=0),
    )(w, avg, total.reshape(experts, 1, width))


def columns(pieces):
    n, experts, depth, width = pieces.shape
    return exchange(pieces).transpose(1, 0, 2, 3).reshape(experts, n * depth, width)


def join_kernel(in_ref, out_ref):
    n, _, _, depth = in_ref.shape
    for k in range(n):
        out_ref[0, :, k * depth : (k + 1) * depth] = in_ref[k, 0]


def rows(x):
    n = lax.axis_size("fsdp")
    experts, height, depth = x.shape
    part = height // n
    pieces = exchange(x.reshape(experts, n, part, depth).transpose(1, 0, 2, 3))
    return pl.pallas_call(
        join_kernel,
        grid=(experts,),
        in_specs=[pl.BlockSpec((n, 1, part, depth), lambda e: (0, e, 0, 0))],
        out_specs=pl.BlockSpec((1, part, n * depth), lambda e: (e, 0, 0)),
        out_shape=jax.ShapeDtypeStruct((experts, part, n * depth), x.dtype),
        cost_estimate=pl.CostEstimate(flops=0, bytes_accessed=4 * x.size, transcendentals=0),
    )(pieces)


def on_device(w_gate, avg_gate, w_up, avg_up, w_down, avg_down, router_weight, router_gain):
    part_router = (router_weight * router_gain[:, None]).astype(jnp.bfloat16)
    row_router = lax.all_gather(part_router, "fsdp", axis=0, tiled=True)
    serve_router = lax.all_gather(row_router, "ep", axis=1, tiled=True)
    total_gate = lax.psum(column_squares(w_gate, avg_gate), "fsdp")
    total_gate, serve_router = lax.optimization_barrier((total_gate, serve_router))
    gate = column_pieces(w_gate, avg_gate, total_gate)
    gate, late_up, late_down = lax.optimization_barrier((gate, avg_up, avg_down))
    serve_gate = columns(gate)
    square_up, square_down = column_squares(w_up, late_up), squares(w_down, late_down, 2)
    total_up, total_down = lax.psum((square_up, square_down), "fsdp")
    up = column_pieces(w_up, avg_up, total_up)
    up, total_down = lax.optimization_barrier((up, total_down))
    serve_up = columns(up)
    serve_down = rows(narrow_of(w_down, avg_down, total_down, 2))

    def own(total, width):
        return jnp.sqrt(
            lax.dynamic_slice_in_dim(total, lax.axis_index("fsdp") * width, width, axis=1)
        )

    scale_gate = own(total_gate, serve_gate.shape[2])
    scale_up = own(total_up, serve_up.shape[2])
    scale_down = own(total_down, serve_down.shape[1])
    return (serve_gate, serve_up, serve_down, scale_gate, scale_up, scale_down, serve_router)


def solution(mesh):
    placed = (
        P("ep", "fsdp", None),
        P("ep", "fsdp", None),
        P("ep", "fsdp", None),
        P("ep", "fsdp", None),
        P("ep", None, "fsdp"),
        P("ep", None, "fsdp"),
        P("fsdp", "ep"),
        P("fsdp"),
    )
    return jax.shard_map(
        on_device,
        mesh=mesh,
        in_specs=placed,
        out_specs=(
            P("ep", None, "fsdp"),
            P("ep", None, "fsdp"),
            P("ep", "fsdp", None),
            P("ep", "fsdp"),
            P("ep", "fsdp"),
            P("ep", "fsdp"),
            P(),
        ),
        check_vma=False,
    )
```
